32 devices in a mesh: dp: 2 (over x), dm: 4 (over z), tp: 4 (over y, core).
Axes of the slice: x: 2, y: 2, z: 4, core: 2. Of those that a mesh axis runs over, the one named last changes fastest.
Arguments:
- hidden: bfloat16 [128, 3072], P('dp', 'dm'), parts along dimension 0
- w_q: bfloat16 [3072, 24, 128], P('dm', 'tp')
- w_k: bfloat16 [3072, 8, 128], P('dm', 'tp')
- w_v: bfloat16 [3072, 8, 128], P('dm', 'tp')
- w_o: bfloat16 [24, 128, 3072], P('tp', None, 'dm')
- w_gate: bfloat16 [3072, 8192], P('dm', 'tp')
- w_up: bfloat16 [3072, 8192], P('dm', 'tp')
- w_down: bfloat16 [8192, 3072], P('tp', 'dm')
- norm_attn: bfloat16 [3072], P('dm')
- norm_mlp: bfloat16 [3072], P('dm')
- k_cache: bfloat16 [128, 1024, 8, 128], P(('dp', 'dm'), None, 'tp'), parts along dimension 0
- v_cache: bfloat16 [128, 1024, 8, 128], P(('dp', 'dm'), None, 'tp'), parts along dimension 0
- seq_lens: int32 [128], P(('dp', 'dm')), parts along dimension 0
- rope_cos: float32 [128, 64], P(('dp', 'dm')), parts along dimension 0
- rope_sin: float32 [128, 64], P(('dp', 'dm')), parts along dimension 0
Outputs:
- output 1: bfloat16 [128, 3072], P('dp', 'dm'), parts along dimension 0
- output 2: bfloat16 [128, 1024, 8, 128], P(('dp', 'dm'), None, 'tp'), parts along dimension 0
- output 3: bfloat16 [128, 1024, 8, 128], P(('dp', 'dm'), None, 'tp'), parts along dimension 0
There are 2 independent parts. The reference program is written for one: setup_inputs(seed, part) draws one part's arguments, and reference() takes and returns one part's arrays. A program takes and returns all parts, laid end to end along the dimension named above; an argument that names none is the same for every part.
All inputs are finite; a program needn't handle non-finite values.
Results may differ from the reference program's by a relative error of at most 0.0107316.
Values are sent between devices in bfloat16 or wider.
A program may use at most 1 GiB of HBM per device.

```python
import math
import jax
import jax.numpy as jnp
from jax import lax

D = 3072
HEADS = 24
KV_HEADS = 8
HEAD = 128
FF = 8192
BATCH = 64
SEQ = 1024

GROUP = HEADS // KV_HEADS
HALF = HEAD // 2
EPS = 1e-6
ROPE_BASE = 10000.0
K_SCALE = math.sqrt(max(math.log(SEQ / 16.0), 1.0))


def rope_tables(seq_lens):
    inv_freq = ROPE_BASE ** (-2.0 * jnp.arange(HALF, dtype=jnp.float32) / HEAD)
    angles = seq_lens.astype(jnp.float32)[:, None] * inv_freq[None, :]
    return jnp.cos(angles), jnp.sin(angles)


def draw_lengths(key):
    lengths = jax.random.randint(key, (BATCH,), SEQ // 8, SEQ, dtype=jnp.int32)
    return lengths.at[0].set(SEQ - 1).at[BATCH - 1].set(SEQ // 8)


def setup_inputs(seed: int = 0, part: int = 0) -> dict:
    shared = jax.random.split(jax.random.key(seed), 9)
    local = jax.random.split(jax.random.fold_in(jax.random.key(seed), part), 4)
    w_q = (jax.random.normal(shared[0], (D, HEADS, HEAD), jnp.float32) * D ** -0.5).astype(jnp.bfloat16)
    w_k = (jax.random.normal(shared[1], (D, KV_HEADS, HEAD), jnp.float32) * (K_SCALE * D ** -0.5)).astype(jnp.bfloat16)
    w_v = (jax.random.normal(shared[2], (D, KV_HEADS, HEAD), jnp.float32) * D ** -0.5).astype(jnp.bfloat16)
    w_o = (jax.random.normal(shared[3], (HEADS, HEAD, D), jnp.float32) * (HEADS * HEAD) ** -0.5).astype(jnp.bfloat16)
    w_gate = (jax.random.normal(shared[4], (D, FF), jnp.float32) * D ** -0.5).astype(jnp.bfloat16)
    w_up = (jax.random.normal(shared[5], (D, FF), jnp.float32) * D ** -0.5).astype(jnp.bfloat16)
    w_down = (jax.random.normal(shared[6], (FF, D), jnp.float32) * FF ** -0.5).astype(jnp.bfloat16)
    norm_attn = (1.0 + 0.4 * jax.random.normal(shared[7], (D,), jnp.float32)).astype(jnp.bfloat16)
    norm_mlp = (1.0 + 0.4 * jax.random.normal(shared[8], (D,), jnp.float32)).astype(jnp.bfloat16)
    hidden = jax.random.normal(local[0], (BATCH, D), jnp.float32).astype(jnp.bfloat16)
    k_cache = (jax.random.normal(local[1], (BATCH, SEQ, KV_HEADS, HEAD), jnp.float32) * K_SCALE).astype(jnp.bfloat16)
    v_cache = jax.random.normal(local[2], (BATCH, SEQ, KV_HEADS, HEAD), jnp.float32).astype(jnp.bfloat16)
    seq_lens = draw_lengths(local[3])
    rope_cos, rope_sin = rope_tables(seq_lens)
    return dict(hidden=hidden, w_q=w_q, w_k=w_k, w_v=w_v, w_o=w_o, w_gate=w_gate, w_up=w_up, w_down=w_down, norm_attn=norm_attn, norm_mlp=norm_mlp, k_cache=k_cache, v_cache=v_cache, seq_lens=seq_lens, rope_cos=rope_cos, rope_sin=rope_sin)


def rms_norm(x, gain):
    x_f32 = x.astype(jnp.float32)
    scale = lax.rsqrt(jnp.mean(x_f32 * x_f32, axis=-1, keepdims=True) + EPS)
    return (x_f32 * scale * gain.astype(jnp.float32)).astype(jnp.bfloat16)


def apply_rope(x, rope_cos, rope_sin):
    first = x[..., :HALF]
    second = x[..., HALF:]
    cosine = rope_cos[:, None, :]
    sine = rope_sin[:, None, :]
    return jnp.concatenate([first * cosine - second * sine, second * cosine + first * sine], axis=-1).astype(jnp.bfloat16)


def project(x, weight):
    return jnp.dot(x, weight.reshape(D, -1), preferred_element_type=jnp.float32).reshape(BATCH, -1, HEAD)


def attend_row(row_args):
    q_row, k_row, v_row, length = row_args
    q_grp = q_row.reshape(KV_HEADS, GROUP, HEAD).astype(jnp.float32)
    scores = jnp.einsum('kgd,skd->kgs', q_grp, k_row.astype(jnp.float32)) / math.sqrt(HEAD)
    key_mask = jnp.arange(SEQ)[None, None, :] <= length
    scores = jnp.where(key_mask, scores, -1e30)
    attn_probs = jax.nn.softmax(scores, axis=-1).astype(jnp.bfloat16).astype(jnp.float32)
    heads = jnp.einsum('kgs,skd->kgd', attn_probs, v_row.astype(jnp.float32))
    return heads.reshape(HEADS, HEAD).astype(jnp.bfloat16)


def reference(hidden, w_q, w_k, w_v, w_o, w_gate, w_up, w_down, norm_attn, norm_mlp, k_cache, v_cache, seq_lens, rope_cos, rope_sin):
    x_norm = rms_norm(hidden, norm_attn)
    q_rot = apply_rope(project(x_norm, w_q), rope_cos, rope_sin)
    k_rot = apply_rope(project(x_norm, w_k), rope_cos, rope_sin)
    v_new = project(x_norm, w_v).astype(jnp.bfloat16)
    write_mask = (jnp.arange(SEQ)[None, :] == seq_lens[:, None])[:, :, None, None]
    k_out = jnp.where(write_mask, k_rot[:, None], k_cache)
    v_out = jnp.where(write_mask, v_new[:, None], v_cache)
    attn_heads = lax.map(attend_row, (q_rot, k_out, v_out, seq_lens))
    attn_out = jnp.dot(attn_heads.reshape(BATCH, HEADS * HEAD), w_o.reshape(HEADS * HEAD, D), preferred_element_type=jnp.float32).astype(jnp.bfloat16)
    h_mid = hidden + attn_out
    x_mlp = rms_norm(h_mid, norm_mlp)
    gate = jnp.dot(x_mlp, w_gate, preferred_element_type=jnp.float32)
    up_proj = jnp.dot(x_mlp, w_up, preferred_element_type=jnp.float32)
    gated_act = (jax.nn.silu(gate) * up_proj).astype(jnp.bfloat16)
    mlp_out = jnp.dot(gated_act, w_down, preferred_element_type=jnp.float32).astype(jnp.bfloat16)
    return (h_mid + mlp_out, k_out, v_out)
```

```python
import jax
import jax.numpy as jnp
from jax import lax
from jax.experimental import pallas as pl
from jax.experimental.pallas import tpu as pltpu
from jax.sharding import PartitionSpec as P

EPS = 1e-6
F32 = jnp.float32
BF16 = jnp.bfloat16
MESH = pl.DeviceIdType.MESH
ANY = pl.BlockSpec(memory_space=pl.ANY)
VM = pl.BlockSpec(memory_space=pltpu.VMEM)
SM = pl.BlockSpec(memory_space=pltpu.SMEM)
DMA = pltpu.SemaphoreType.DMA

NZ = 4
NT = 4
ROWS = 64
RB = 16
W = 768
HD = 128
NH = 6
GRP = 3
SEQ2 = 2048
QKV = (NH + 4) * HD
PAY = QKV + HD
FFL = 2048
NP = 8
PC = 128


def partners(i):
    return (3 - i, (i + 2) % 4, i + 1 - 2 * (i % 2))


def dot(a, b):
    return jnp.dot(a, b, preferred_element_type=F32)


def local_scale(x, width):
    ss = jnp.sum(x * x, axis=-1, keepdims=True)
    return ss, lax.rsqrt(ss / width + EPS)


def qkv_kernel(hid, gain, wq, wk, wv, cos, sin, kc, vc,
               q_o, k_o, v_o, kc_o, vc_o,
               h_s, g_s, wq_s, wk_s, wv_s, cos_s, sin_s, part, recv,
               in_sem, c_sem, send_sem, recv_sem):
    z = lax.axis_index('dm')
    peers = partners(z)
    ins = [pltpu.make_async_copy(s, d, in_sem.at[i]) for i, (s, d) in enumerate(
        ((hid, h_s), (gain, g_s), (wk, wk_s), (wv, wv_s), (wq, wq_s), (cos, cos_s), (sin, sin_s)))]
    for c in ins:
        c.start()
    caches = [pltpu.make_async_copy(kc, kc_o, c_sem.at[0]), pltpu.make_async_copy(vc, vc_o, c_sem.at[1])]
    for c in caches:
        c.start()
    barrier = pltpu.get_barrier_semaphore()
    for p in peers:
        pl.semaphore_signal(barrier, inc=1, device_id={'dm': p}, device_id_type=MESH)

    ins[0].wait()
    ins[1].wait()
    h = h_s[...].astype(F32)
    ss, scale = local_scale(h, W)
    part[:, QKV:PAY] = jnp.broadcast_to(ss, (ROWS, HD))
    x = (h * scale * g_s[...].astype(F32).reshape(1, W)).astype(BF16)
    rr = lax.broadcasted_iota(jnp.int32, (HD, 2 * HD), 0)
    cc = lax.broadcasted_iota(jnp.int32, (HD, 2 * HD), 1)
    spread = []
    for hd in range(2):
        sel = jnp.where(cc == 2 * rr + hd, 1.0, 0.0).astype(BF16)
        spread.append(jnp.concatenate(
            [dot(x[:, j * HD:(j + 1) * HD], sel).astype(BF16) for j in range(W // HD)], axis=1))
    xe = jnp.concatenate(spread, axis=0)
    ins[2].wait()
    kk = dot(xe, wk_s[...])
    ins[3].wait()
    vv = dot(xe, wv_s[...])
    for hd in range(2):
        part[:, (NH + hd) * HD:(NH + hd + 1) * HD] = kk[hd * ROWS:(hd + 1) * ROWS]
        part[:, (NH + 2 + hd) * HD:(NH + 3 + hd) * HD] = vv[hd * ROWS:(hd + 1) * ROWS]
    ins[4].wait()
    for hd in range(NH):
        part[:, hd * HD:(hd + 1) * HD] = dot(x, wq_s[hd])
    pl.semaphore_wait(barrier, NZ - 1)
    copies = []
    for k, p in enumerate(peers):
        c = pltpu.make_async_remote_copy(
            src_ref=part.at[pl.ds(pl.multiple_of(p * RB, RB), RB)], dst_ref=recv.at[k], send_sem=send_sem.at[k], recv_sem=recv_sem.at[k],
            device_id={'dm': p}, device_id_type=MESH)
        c.start()
        copies.append(c)
    ins[5].wait()
    ins[6].wait()
    own = part[pl.ds(pl.multiple_of(z * RB, RB), RB), :]
    for c in copies:
        c.wait_recv()
    parts = [own] + [recv[k] for k in range(NZ - 1)]
    stats = [t[:, QKV:PAY] for t in parts]
    glob = lax.rsqrt((stats[0] + stats[1] + stats[2] + stats[3]) / (NZ * W) + EPS)
    ratio = [glob * jnp.sqrt(s / W + EPS) for s in stats]

    def head(i):
        cols = slice(i * HD, (i + 1) * HD)
        return sum(t[:, cols] * r for t, r in zip(parts, ratio))

    cs = jnp.concatenate([cos_s[...], cos_s[...]], axis=1)
    sn = jnp.concatenate([-sin_s[...], sin_s[...]], axis=1)

    def rope(t):
        return (t * cs + pltpu.roll(t, HD // 2, 1) * sn).astype(BF16).astype(F32)

    for i in range(NH):
        q_o[:, i, :] = rope(head(i))
    for i in range(NH, 8):
        q_o[:, i, :] = jnp.zeros((RB, HD), F32)
    for hd in range(2):
        kn = rope(head(NH + hd))
        vn = head(NH + 2 + hd).astype(BF16).astype(F32)
        for r in range(hd, 8, 2):
            k_o[:, r, :] = kn
            v_o[:, r, :] = vn
    for c in copies:
        c.wait_send()
    for c in caches:
        c.wait()


def attn_kernel(lens, q, kn, vn, kc, vc, o, k_out, v_out, kc_a, vc_a, o_s, sem):
    del kc, vc
    r16 = lax.broadcasted_iota(jnp.int32, (16, HD), 0)
    writes = []
    for b in range(RB):
        ln = lens[b]
        base = pl.multiple_of(b * SEQ2 + (ln // 8) * 16, 16)
        hit = (r16 // 2) == (ln % 8)
        for j, (new, cache, out) in enumerate(((kn, kc_a, k_out), (vn, vc_a, v_out))):
            fresh = jnp.concatenate([new[b], new[b]], axis=0)
            tile = cache[pl.ds(base, 16), :].astype(F32)
            cache[pl.ds(base, 16), :] = jnp.where(hit, fresh, tile).astype(BF16)
            rows = pl.ds(b * SEQ2, SEQ2)
            w = pltpu.make_async_copy(cache.at[rows], out.at[rows], sem.at[j, b])
            w.start()
            writes.append(w)
    row = lax.broadcasted_iota(jnp.int32, (16, SEQ2), 0)
    col = lax.broadcasted_iota(jnp.int32, (16, SEQ2), 1)
    same_head = (col % 2) == jnp.where(row % 8 < GRP, 0, 1)
    slot = jnp.where(same_head, col // 2, SEQ2)
    zero = jnp.zeros((8, HD), F32)
    row1 = lax.broadcasted_iota(jnp.int32, (16, 1), 0)
    for b in range(0, RB, 2):
        lhs = jnp.concatenate([jnp.concatenate([q[b], zero], axis=1),
                               jnp.concatenate([zero, q[b + 1]], axis=1)], axis=0).astype(BF16)
        r0, r1 = pl.ds(b * SEQ2, SEQ2), pl.ds((b + 1) * SEQ2, SEQ2)
        kk = jnp.concatenate([kc_a[r0, :], kc_a[r1, :]], axis=1)
        s = lax.dot_general(lhs, kk, (((1,), (1,)), ((), ())), preferred_element_type=F32)
        ln = jnp.where(row1 < 8, lens[b], lens[b + 1])
        s = jnp.where(slot <= ln, s * (HD ** -0.5), -1e30)
        e = jnp.exp(s - jnp.max(s, axis=1, keepdims=True))
        pr = (e * (1.0 / jnp.sum(e, axis=1, keepdims=True))).astype(BF16)
        vv = jnp.concatenate([vc_a[r0, :], vc_a[r1, :]], axis=1)
        oo = dot(pr, vv)
        o_s[b] = oo[:8, :HD]
        o_s[b + 1] = oo[8:, HD:]
    for hd in range(NH):
        o[:, hd * HD:(hd + 1) * HD] = o_s[:, hd, :].astype(BF16)
    for w in writes:
        w.wait()


def tail_kernel(o, hid, gain, w_o, w_g, w_u, w_d, out,
                o_all, h_s, g_s, wo_s, wg_s, wu_s, wd_s, part, rs_recv, h1_all, st_send, st_recv,
                nsend, fsend, nrecv, frecv, m_all, part2, rs2_recv, ho_all,
                w_sem, o_send, o_recv, rs_send, rs_rcv, h1_send, h1_recv, st_ss, st_rs,
                ns_sem, fs_sem, nr_sem, fr_sem, m_send, m_recv, rs2_send, rs2_rcv, ho_send, ho_recv):
    z = lax.axis_index('dm')
    t = lax.axis_index('tp')
    zp, tp = partners(z), partners(t)
    loads = [pltpu.make_async_copy(s, d, w_sem.at[i]) for i, (s, d) in enumerate(
        ((w_o, wo_s), (hid, h_s), (gain, g_s), (w_g, wg_s), (w_u, wu_s), (w_d, wd_s)))]
    for c in loads:
        c.start()
    barrier = pltpu.get_barrier_semaphore()
    for p in zp:
        pl.semaphore_signal(barrier, inc=1, device_id={'dm': p}, device_id_type=MESH)
    for p in tp:
        pl.semaphore_signal(barrier, inc=1, device_id={'tp': p}, device_id_type=MESH)
    pl.semaphore_wait(barrier, 6)

    def remote(src, dst, ss, rs, dev):
        c = pltpu.make_async_remote_copy(src_ref=src, dst_ref=dst, send_sem=ss, recv_sem=rs, device_id=dev, device_id_type=MESH)
        c.start()
        return c

    def my(i):
        return pl.ds(pl.multiple_of(i * RB, RB), RB)

    pending = []
    cps = [remote(o, o_all.at[k], o_send.at[k], o_recv.at[k], {'dm': p}) for k, p in enumerate(zp)]
    pending += cps
    loads[0].wait()
    part[my(z), :] = dot(o[...], wo_s[...])
    for k in (2, 1, 0):
        cps[k].wait_recv()
        part[my(zp[k]), :] = dot(o_all[k], wo_s[...])

    def tp_scatter(buf, recv, ss, rs):
        cs = [remote(buf.at[my(p)], recv.at[k], ss.at[k], rs.at[k], {'tp': p}) for k, p in enumerate(tp)]
        tot = buf[my(t), :]
        for k in (2, 1, 0):
            cs[k].wait_recv()
            tot = tot + recv[k]
        pending.extend(cs)
        return tot

    def tp_gather(buf, ss, rs):
        cs = [remote(buf.at[my(t)], buf.at[my(t)], ss.at[k], rs.at[k], {'tp': p}) for k, p in enumerate(tp)]
        for c in cs:
            c.wait_recv()
        pending.extend(cs)

    tot = tp_scatter(part, rs_recv, rs_send, rs_rcv)
    loads[1].wait()
    h1 = (h_s[my(t), :].astype(F32) + tot.astype(BF16).astype(F32)).astype(BF16)
    h1_all[my(t), :] = h1
    tp_gather(h1_all, h1_send, h1_recv)
    hf = h1_all[...].astype(F32)
    ss, scale = local_scale(hf, W)
    ssb = jnp.broadcast_to(ss, (ROWS, HD))
    st_send[...] = jnp.transpose(ssb)[:8, :]
    scp = [remote(st_send, st_recv.at[k], st_ss.at[k], st_rs.at[k], {'dm': p}) for k, p in enumerate(zp)]
    pending += scp
    loads[2].wait()
    x2 = (hf * scale * g_s[...].astype(F32).reshape(1, W)).astype(BF16)
    loads[3].wait()
    loads[4].wait()

    nd = z // 2
    end = (z % 3) == 0
    mid = jnp.logical_not(end)
    step = 1 - 2 * nd
    near_dst, far_dst = z + step, z - step
    near_ok, far_ok = {'dm': lax.rem(near_dst + NZ, NZ)}, {'dm': lax.rem(far_dst + NZ, NZ)}

    def piece(c):
        cols = pl.ds(pl.multiple_of(c * PC, PC), PC)
        return dot(x2, jnp.concatenate([wg_s[:, cols], wu_s[:, cols]], axis=1))

    def near_copy(i, dst, rsem):
        return pltpu.make_async_remote_copy(src_ref=nsend.at[i], dst_ref=dst.at[i], send_sem=ns_sem.at[i], recv_sem=rsem.at[i],
                                            device_id=near_ok, device_id_type=MESH)

    def far_copy(i):
        return pltpu.make_async_remote_copy(src_ref=fsend.at[i], dst_ref=frecv.at[i], send_sem=fs_sem.at[i], recv_sem=fr_sem.at[i],
                                            device_id=far_ok, device_id_type=MESH)

    def m_copies(i):
        cb = (1 - nd) * NP + i
        return [pltpu.make_async_remote_copy(src_ref=m_all.at[cb], dst_ref=m_all.at[cb], send_sem=m_send.at[k, i], recv_sem=m_recv.at[cb],
                                             device_id={'dm': p}, device_id_type=MESH) for k, p in enumerate(zp)]

    @pl.when(end)
    def _():
        for i in range(NP):
            nsend[i] = piece(nd * NP + i)
            near_copy(i, nrecv, nr_sem).start()

    for c in scp:
        c.wait_recv()

    def col(row8):
        return jnp.transpose(jnp.broadcast_to(row8[0:1, :], (HD, ROWS)))

    sts = [col(st_recv[k]) for k in range(NZ - 1)]
    glob = lax.rsqrt((ssb + sts[0] + sts[1] + sts[2]) / (NZ * W) + EPS)
    r_me = glob * jnp.sqrt(ssb / W + EPS)
    r_end = glob * jnp.sqrt(sts[2] / W + EPS)
    r_me2 = jnp.concatenate([r_me, r_me], axis=1)
    r_end2 = jnp.concatenate([r_end, r_end], axis=1)

    @pl.when(mid)
    def _():
        def near(i):
            mine = piece(nd * NP + i) * r_me2
            near_copy(i, nrecv, nr_sem).wait_recv()
            nsend[i] = nrecv[i] * r_end2 + mine
            near_copy(i, frecv, fr_sem).start()

        def far(i):
            mine = piece((1 - nd) * NP + i) * r_me2
            far_copy(i).wait_recv()
            fsend[i] = frecv[i] + mine
            far_copy(i).start()

        for i in range(NP + 2):
            if i < NP:
                near(i)
            if i >= 2:
                far(i - 2)

    @pl.when(end)
    def _():
        for i in range(NP):
            mine = piece((1 - nd) * NP + i) * r_me2
            far_copy(i).wait_recv()
            tot = frecv[i] + mine
            gate, up = tot[:, :PC], tot[:, PC:]
            m_all[(1 - nd) * NP + i] = (gate * (1.0 / (1.0 + jnp.exp(-gate))) * up).astype(BF16)
            for c in m_copies(i):
                c.start()

    def m_wait(cb, i):
        pltpu.make_async_remote_copy(src_ref=m_all.at[cb], dst_ref=m_all.at[cb], send_sem=m_send.at[0, i], recv_sem=m_recv.at[cb],
                                     device_id={'dm': zp[0]}, device_id_type=MESH).wait_recv()

    loads[5].wait()
    for i in range(NP):
        m_wait(nd * NP + i, i)

        @pl.when(mid)
        def _():
            m_wait((1 - nd) * NP + i, i)

    acc = None
    for j in range(NP):
        d = dot(jnp.concatenate([m_all[2 * j], m_all[2 * j + 1]], axis=1), wd_s[2 * j * PC:2 * (j + 1) * PC, :])
        acc = d if acc is None else acc + d
    part2[...] = acc
    tot = tp_scatter(part2, rs2_recv, rs2_send, rs2_rcv)
    ho_all[my(t), :] = (h1_all[my(t), :].astype(F32) + tot.astype(BF16).astype(F32)).astype(BF16)
    tp_gather(ho_all, ho_send, ho_recv)
    out[...] = ho_all[...]
    for c in pending:
        c.wait_send()

    @pl.when(end)
    def _():
        for i in range(NP):
            near_copy(i, nrecv, nr_sem).wait_send()
            for c in m_copies(i):
                c.wait_send()

    @pl.when(mid)
    def _():
        for i in range(NP):
            near_copy(i, frecv, fr_sem).wait_send()
            far_copy(i).wait_send()


def local_layer(hidden, w_q, w_k, w_v, w_o, w_gate, w_up, w_down, norm_attn, norm_mlp, k_cache, v_cache, seq_lens, rope_cos, rope_sin):
    mib = 1 << 20
    kc = k_cache.reshape(RB * SEQ2, HD)
    vc = v_cache.reshape(RB * SEQ2, HD)
    q, kn, vn, kc, vc = pl.pallas_call(
        qkv_kernel,
        out_shape=(pltpu.VMEM((RB, 8, HD), F32), pltpu.VMEM((RB, 8, HD), F32), pltpu.VMEM((RB, 8, HD), F32),
                   pltpu.VMEM((RB * SEQ2, HD), BF16), pltpu.VMEM((RB * SEQ2, HD), BF16)),
        in_specs=[ANY] * 9,
        out_specs=(VM,) * 5,
        scratch_shapes=[
            pltpu.VMEM((ROWS, W), BF16), pltpu.VMEM((W,), BF16), pltpu.VMEM((NH, W, HD), BF16),
            pltpu.VMEM((2 * W, HD), BF16), pltpu.VMEM((2 * W, HD), BF16), pltpu.VMEM((RB, HD // 2), F32), pltpu.VMEM((RB, HD // 2), F32),
            pltpu.VMEM((ROWS, PAY), F32), pltpu.VMEM((NZ - 1, RB, PAY), F32),
            DMA((7,)), DMA((2,)), DMA((3,)), DMA((3,))],
        compiler_params=pltpu.CompilerParams(collective_id=0, has_side_effects=True, vmem_limit_bytes=40 * mib),
        name='qkv',
    )(hidden, norm_attn, w_q.transpose(1, 0, 2), w_k.reshape(2 * W, HD), w_v.reshape(2 * W, HD), rope_cos, rope_sin, kc, vc)

    o, k_out, v_out, _, _ = pl.pallas_call(
        attn_kernel,
        out_shape=(pltpu.VMEM((RB, W), BF16), jax.ShapeDtypeStruct((RB * SEQ2, HD), BF16), jax.ShapeDtypeStruct((RB * SEQ2, HD), BF16),
                   pltpu.VMEM((RB * SEQ2, HD), BF16), pltpu.VMEM((RB * SEQ2, HD), BF16)),
        in_specs=[SM, VM, VM, VM, VM, VM],
        out_specs=(VM, ANY, ANY, VM, VM),
        scratch_shapes=[pltpu.VMEM((RB, 8, HD), F32), DMA((2, RB))],
        input_output_aliases={4: 3, 5: 4},
        compiler_params=pltpu.CompilerParams(vmem_limit_bytes=40 * mib),
        name='attn',
    )(seq_lens, q, kn, vn, kc, vc)

    h_out = pl.pallas_call(
        tail_kernel,
        out_shape=jax.ShapeDtypeStruct((ROWS, W), BF16),
        in_specs=[VM] + [ANY] * 6,
        out_specs=VM,
        scratch_shapes=[
            pltpu.VMEM((NZ - 1, RB, W), BF16), pltpu.VMEM((ROWS, W), BF16), pltpu.VMEM((W,), BF16),
            pltpu.VMEM((W, W), BF16), pltpu.VMEM((W, FFL), BF16), pltpu.VMEM((W, FFL), BF16), pltpu.VMEM((FFL, W), BF16),
            pltpu.VMEM((ROWS, W), F32), pltpu.VMEM((NT - 1, RB, W), F32), pltpu.VMEM((ROWS, W), BF16),
            pltpu.VMEM((8, ROWS), F32), pltpu.VMEM((NZ - 1, 8, ROWS), F32),
            pltpu.VMEM((NP, ROWS, 2 * PC), F32), pltpu.VMEM((NP, ROWS, 2 * PC), F32), pltpu.VMEM((NP, ROWS, 2 * PC), F32),
            pltpu.VMEM((NP, ROWS, 2 * PC), F32), pltpu.VMEM((2 * NP, ROWS, PC), BF16),
            pltpu.VMEM((ROWS, W), F32), pltpu.VMEM((NT - 1, RB, W), F32), pltpu.VMEM((ROWS, W), BF16),
            DMA((6,)), DMA((3,)), DMA((3,)), DMA((3,)), DMA((3,)), DMA((3,)), DMA((3,)), DMA((3,)), DMA((3,)),
            DMA((NP,)), DMA((NP,)), DMA((NP,)), DMA((NP,)), DMA((3, NP)), DMA((2 * NP,)), DMA((3,)), DMA((3,)), DMA((3,)), DMA((3,))],
        compiler_params=pltpu.CompilerParams(collective_id=1, has_side_effects=True, vmem_limit_bytes=40 * mib),
        name='tail',
    )(o, hidden, norm_mlp, w_o.reshape(W, W), w_gate, w_up, w_down)
    shape = (RB, SEQ2 // 2, 2, HD)
    return h_out, k_out.reshape(shape), v_out.reshape(shape)


def solution(mesh):
    row_spec = P('dp', 'dm')
    cache_spec = P(('dp', 'dm'), None, 'tp', None)
    batch_spec = P(('dp', 'dm'))
    rope_spec = P(('dp', 'dm'), None)
    in_specs = (row_spec, P('dm', 'tp', None), P('dm', 'tp', None), P('dm', 'tp', None), P('tp', None, 'dm'), P('dm', 'tp'), P('dm', 'tp'), P('tp', 'dm'), P('dm'), P('dm'), cache_spec, cache_spec, batch_spec, rope_spec, rope_spec)
    return jax.shard_map(local_layer, mesh=mesh, in_specs=in_specs, out_specs=(row_spec, cache_spec, cache_spec), check_vma=False)
```

```python
import jax
import jax.numpy as jnp
from jax import lax
from jax.experimental import pallas as pl
from jax.experimental.pallas import tpu as pltpu
from jax.sharding import PartitionSpec as P

EPS = 1e-6
F32 = jnp.float32
BF16 = jnp.bfloat16
MESH = pl.DeviceIdType.MESH
ANY = pl.BlockSpec(memory_space=pl.ANY)
VM = pl.BlockSpec(memory_space=pltpu.VMEM)
SM = pl.BlockSpec(memory_space=pltpu.SMEM)
DMA = pltpu.SemaphoreType.DMA

NZ = 4
NT = 4
ROWS = 64
RB = 16
W = 768
HD = 128
NH = 6
GRP = 3
SEQ2 = 2048
QKV = (NH + 4) * HD
PAY = QKV + HD
FFL = 2048
NP = 8
PC = 128


def partners(i):
    return (3 - i, (i + 2) % 4, i + 1 - 2 * (i % 2))


def dot(a, b):
    return jnp.dot(a, b, preferred_element_type=F32)


def local_scale(x, width):
    ss = jnp.sum(x * x, axis=-1, keepdims=True)
    return ss, lax.rsqrt(ss / width + EPS)


def qkv_kernel(hid, gain, wq, wk, wv, cos, sin, kc, vc,
               q_o, k_o, v_o, kc_o, vc_o,
               h_s, g_s, wq_s, wk_s, wv_s, cos_s, sin_s, part, recv,
               in_sem, c_sem, send_sem, recv_sem):
    z = lax.axis_index('dm')
    peers = partners(z)
    ins = [pltpu.make_async_copy(s, d, in_sem.at[i]) for i, (s, d) in enumerate(
        ((hid, h_s), (gain, g_s), (wk, wk_s), (wv, wv_s), (wq, wq_s), (cos, cos_s), (sin, sin_s)))]
    for c in ins:
        c.start()
    caches = [pltpu.make_async_copy(kc, kc_o, c_sem.at[0]), pltpu.make_async_copy(vc, vc_o, c_sem.at[1])]
    for c in caches:
        c.start()
    barrier = pltpu.get_barrier_semaphore()
    for p in peers:
        pl.semaphore_signal(barrier, inc=1, device_id={'dm': p}, device_id_type=MESH)

    ins[0].wait()
    ins[1].wait()
    h = h_s[...].astype(F32)
    ss, scale = local_scale(h, W)
    part[:, QKV:PAY] = jnp.broadcast_to(ss, (ROWS, HD))
    x = (h * scale * g_s[...].astype(F32).reshape(1, W)).astype(BF16)
    rr = lax.broadcasted_iota(jnp.int32, (HD, 2 * HD), 0)
    cc = lax.broadcasted_iota(jnp.int32, (HD, 2 * HD), 1)
    spread = []
    for hd in range(2):
        sel = jnp.where(cc == 2 * rr + hd, 1.0, 0.0).astype(BF16)
        spread.append(jnp.concatenate(
            [dot(x[:, j * HD:(j + 1) * HD], sel).astype(BF16) for j in range(W // HD)], axis=1))
    xe = jnp.concatenate(spread, axis=0)
    ins[2].wait()
    kk = dot(xe, wk_s[...])
    ins[3].wait()
    vv = dot(xe, wv_s[...])
    for hd in range(2):
        part[:, (NH + hd) * HD:(NH + hd + 1) * HD] = kk[hd * ROWS:(hd + 1) * ROWS]
        part[:, (NH + 2 + hd) * HD:(NH + 3 + hd) * HD] = vv[hd * ROWS:(hd + 1) * ROWS]
    ins[4].wait()
    for hd in range(NH):
        part[:, hd * HD:(hd + 1) * HD] = dot(x, wq_s[hd])
    pl.semaphore_wait(barrier, NZ - 1)
    copies = []
    for k, p in enumerate(peers):
        c = pltpu.make_async_remote_copy(
            src_ref=part.at[pl.ds(pl.multiple_of(p * RB, RB), RB)], dst_ref=recv.at[k], send_sem=send_sem.at[k], recv_sem=recv_sem.at[k],
            device_id={'dm': p}, device_id_type=MESH)
        c.start()
        copies.append(c)
    ins[5].wait()
    ins[6].wait()
    own = part[pl.ds(pl.multiple_of(z * RB, RB), RB), :]
    for c in copies:
        c.wait_recv()
    parts = [own] + [recv[k] for k in range(NZ - 1)]
    stats = [t[:, QKV:PAY] for t in parts]
    glob = lax.rsqrt((stats[0] + stats[1] + stats[2] + stats[3]) / (NZ * W) + EPS)
    ratio = [glob * jnp.sqrt(s / W + EPS) for s in stats]

    def head(i):
        cols = slice(i * HD, (i + 1) * HD)
        return sum(t[:, cols] * r for t, r in zip(parts, ratio))

    cs = jnp.concatenate([cos_s[...], cos_s[...]], axis=1)
    sn = jnp.concatenate([-sin_s[...], sin_s[...]], axis=1)

    def rope(t):
        return (t * cs + pltpu.roll(t, HD // 2, 1) * sn).astype(BF16).astype(F32)

    for i in range(NH):
        q_o[:, i, :] = rope(head(i))
    for i in range(NH, 8):
        q_o[:, i, :] = jnp.zeros((RB, HD), F32)
    for hd in range(2):
        kn = rope(head(NH + hd))
        vn = head(NH + 2 + hd).astype(BF16).astype(F32)
        for r in range(hd, 8, 2):
            k_o[:, r, :] = kn
            v_o[:, r, :] = vn
    for c in copies:
        c.wait_send()
    for c in caches:
        c.wait()


def attn_kernel(lens, q, kn, vn, kc, vc, o, k_out, v_out, kc_a, vc_a, o_s, sem):
    del kc, vc
    r16 = lax.broadcasted_iota(jnp.int32, (16, HD), 0)
    writes = []
    for b in range(RB):
        ln = lens[b]
        base = pl.multiple_of(b * SEQ2 + (ln // 8) * 16, 16)
        hit = (r16 // 2) == (ln % 8)
        for j, (new, cache, out) in enumerate(((kn, kc_a, k_out), (vn, vc_a, v_out))):
            fresh = jnp.concatenate([new[b], new[b]], axis=0)
            tile = cache[pl.ds(base, 16), :].astype(F32)
            cache[pl.ds(base, 16), :] = jnp.where(hit, fresh, tile).astype(BF16)
            rows = pl.ds(b * SEQ2, SEQ2)
            w = pltpu.make_async_copy(cache.at[rows], out.at[rows], sem.at[j, b])
            w.start()
            writes.append(w)
    row = lax.broadcasted_iota(jnp.int32, (16, SEQ2), 0)
    col = lax.broadcasted_iota(jnp.int32, (16, SEQ2), 1)
    same_head = (col % 2) == jnp.where(row % 8 < GRP, 0, 1)
    slot = jnp.where(same_head, col // 2, SEQ2)
    zero = jnp.zeros((8, HD), F32)
    row1 = lax.broadcasted_iota(jnp.int32, (16, 1), 0)
    for b in range(0, RB, 2):
        lhs = jnp.concatenate([jnp.concatenate([q[b], zero], axis=1),
                               jnp.concatenate([zero, q[b + 1]], axis=1)], axis=0).astype(BF16)
        r0, r1 = pl.ds(b * SEQ2, SEQ2), pl.ds((b + 1) * SEQ2, SEQ2)
        kk = jnp.concatenate([kc_a[r0, :], kc_a[r1, :]], axis=1)
        s = lax.dot_general(lhs, kk, (((1,), (1,)), ((), ())), preferred_element_type=F32)
        ln = jnp.where(row1 < 8, lens[b], lens[b + 1])
        s = jnp.where(slot <= ln, s * (HD ** -0.5), -1e30)
        e = jnp.exp(s - jnp.max(s, axis=1, keepdims=True))
        pr = (e * (1.0 / jnp.sum(e, axis=1, keepdims=True))).astype(BF16)
        vv = jnp.concatenate([vc_a[r0, :], vc_a[r1, :]], axis=1)
        oo = dot(pr, vv)
        o_s[b] = oo[:8, :HD]
        o_s[b + 1] = oo[8:, HD:]
    for hd in range(NH):
        o[:, hd * HD:(hd + 1) * HD] = o_s[:, hd, :].astype(BF16)
    for w in writes:
        w.wait()


def tail_kernel(o, hid, gain, w_o, w_g, w_u, w_d, out,
                o_all, h_s, g_s, wo_s, wg_s, wu_s, wd_s, part, rs_recv, h1_all, st_send, st_recv,
                nsend, fsend, nrecv, frecv, m_all, part2, rs2_recv, ho_all,
                w_sem, o_send, o_recv, rs_send, rs_rcv, h1_send, h1_recv, st_ss, st_rs,
                ns_sem, fs_sem, nr_sem, fr_sem, m_send, m_recv, rs2_send, rs2_rcv, ho_send, ho_recv):
    z = lax.axis_index('dm')
    t = lax.axis_index('tp')
    zp, tp = partners(z), partners(t)
    loads = [pltpu.make_async_copy(s, d, w_sem.at[i]) for i, (s, d) in enumerate(
        ((w_o, wo_s), (hid, h_s), (gain, g_s), (w_g, wg_s), (w_u, wu_s), (w_d, wd_s)))]
    for c in loads:
        c.start()
    barrier = pltpu.get_barrier_semaphore()
    for p in zp:
        pl.semaphore_signal(barrier, inc=1, device_id={'dm': p}, device_id_type=MESH)
    for p in tp:
        pl.semaphore_signal(barrier, inc=1, device_id={'tp': p}, device_id_type=MESH)
    pl.semaphore_wait(barrier, 6)

    def remote(src, dst, ss, rs, dev):
        c = pltpu.make_async_remote_copy(src_ref=src, dst_ref=dst, send_sem=ss, recv_sem=rs, device_id=dev, device_id_type=MESH)
        c.start()
        return c

    def my(i):
        return pl.ds(pl.multiple_of(i * RB, RB), RB)

    pending = []
    cps = [remote(o, o_all.at[k], o_send.at[k], o_recv.at[k], {'dm': p}) for k, p in enumerate(zp)]
    pending += cps
    loads[0].wait()
    part[my(z), :] = dot(o[...], wo_s[...])
    for k in (2, 1, 0):
        cps[k].wait_recv()
        part[my(zp[k]), :] = dot(o_all[k], wo_s[...])

    def tp_scatter(buf, recv, ss, rs):
        cs = [remote(buf.at[my(p)], recv.at[k], ss.at[k], rs.at[k], {'tp': p}) for k, p in enumerate(tp)]
        tot = buf[my(t), :]
        for k in (2, 1, 0):
            cs[k].wait_recv()
            tot = tot + recv[k]
        pending.extend(cs)
        return tot

    def tp_gather(buf, ss, rs):
        cs = [remote(buf.at[my(t)], buf.at[my(t)], ss.at[k], rs.at[k], {'tp': p}) for k, p in enumerate(tp)]
        for c in cs:
            c.wait_recv()
        pending.extend(cs)

    tot = tp_scatter(part, rs_recv, rs_send, rs_rcv)
    loads[1].wait()
    h1 = (h_s[my(t), :].astype(F32) + tot.astype(BF16).astype(F32)).astype(BF16)
    h1_all[my(t), :] = h1
    tp_gather(h1_all, h1_send, h1_recv)
    hf = h1_all[...].astype(F32)
    ss, scale = local_scale(hf, W)
    ssb = jnp.broadcast_to(ss, (ROWS, HD))
    st_send[...] = jnp.transpose(ssb)[:8, :]
    scp = [remote(st_send, st_recv.at[k], st_ss.at[k], st_rs.at[k], {'dm': p}) for k, p in enumerate(zp)]
    pending += scp
    loads[2].wait()
    x2 = (hf * scale * g_s[...].astype(F32).reshape(1, W)).astype(BF16)
    loads[3].wait()
    loads[4].wait()

    nd = z // 2
    end = (z % 3) == 0
    mid = jnp.logical_not(end)
    step = 1 - 2 * nd
    near_dst, far_dst = z + step, z - step
    near_ok, far_ok = {'dm': lax.rem(near_dst + NZ, NZ)}, {'dm': lax.rem(far_dst + NZ, NZ)}

    def piece(c):
        cols = pl.ds(pl.multiple_of(c * PC, PC), PC)
        return dot(x2, jnp.concatenate([wg_s[:, cols], wu_s[:, cols]], axis=1))

    def near_copy(i, dst, rsem):
        return pltpu.make_async_remote_copy(src_ref=nsend.at[i], dst_ref=dst.at[i], send_sem=ns_sem.at[i], recv_sem=rsem.at[i],
                                            device_id=near_ok, device_id_type=MESH)

    def far_copy(i):
        return pltpu.make_async_remote_copy(src_ref=fsend.at[i], dst_ref=frecv.at[i], send_sem=fs_sem.at[i], recv_sem=fr_sem.at[i],
                                            device_id=far_ok, device_id_type=MESH)

    def m_copies(i):
        cb = (1 - nd) * NP + i
        return [pltpu.make_async_remote_copy(src_ref=m_all.at[cb], dst_ref=m_all.at[cb], send_sem=m_send.at[k, i], recv_sem=m_recv.at[cb],
                                             device_id={'dm': p}, device_id_type=MESH) for k, p in enumerate(zp)]

    @pl.when(end)
    def _():
        for i in range(NP):
            nsend[i] = piece(nd * NP + i)
            near_copy(i, nrecv, nr_sem).start()

    for c in scp:
        c.wait_recv()

    def col(row8):
        return jnp.transpose(jnp.broadcast_to(row8[0:1, :], (HD, ROWS)))

    sts = [col(st_recv[k]) for k in range(NZ - 1)]
    glob = lax.rsqrt((ssb + sts[0] + sts[1] + sts[2]) / (NZ * W) + EPS)
    r_me = glob * jnp.sqrt(ssb / W + EPS)
    r_end = glob * jnp.sqrt(sts[2] / W + EPS)
    r_me2 = jnp.concatenate([r_me, r_me], axis=1)
    r_end2 = jnp.concatenate([r_end, r_end], axis=1)

    @pl.when(mid)
    def _():
        def near(i):
            mine = piece(nd * NP + i) * r_me2
            near_copy(i, nrecv, nr_sem).wait_recv()
            nsend[i] = nrecv[i] * r_end2 + mine
            near_copy(i, frecv, fr_sem).start()

        def far(i):
            mine = piece((1 - nd) * NP + i) * r_me2
            far_copy(i).wait_recv()
            fsend[i] = frecv[i] + mine
            far_copy(i).start()

        for i in range(NP + 2):
            if i < NP:
                near(i)
            if i >= 2:
                far(i - 2)

    @pl.when(end)
    def _():
        for i in range(NP):
            mine = piece((1 - nd) * NP + i) * r_me2
            far_copy(i).wait_recv()
            tot = frecv[i] + mine
            gate, up = tot[:, :PC], tot[:, PC:]
            m_all[(1 - nd) * NP + i] = (gate * (1.0 / (1.0 + jnp.exp(-gate))) * up).astype(BF16)
            for c in m_copies(i):
                c.start()

    def m_wait(cb, i):
        pltpu.make_async_remote_copy(src_ref=m_all.at[cb], dst_ref=m_all.at[cb], send_sem=m_send.at[0, i], recv_sem=m_recv.at[cb],
                                     device_id={'dm': zp[0]}, device_id_type=MESH).wait_recv()

    loads[5].wait()
    for i in range(NP):
        m_wait(nd * NP + i, i)

        @pl.when(mid)
        def _():
            m_wait((1 - nd) * NP + i, i)

    acc = None
    for j in range(NP):
        d = dot(jnp.concatenate([m_all[2 * j], m_all[2 * j + 1]], axis=1), wd_s[2 * j * PC:2 * (j + 1) * PC, :])
        acc = d if acc is None else acc + d
    part2[...] = acc
    tot = tp_scatter(part2, rs2_recv, rs2_send, rs2_rcv)
    ho_all[my(t), :] = (h1_all[my(t), :].astype(F32) + tot.astype(BF16).astype(F32)).astype(BF16)
    tp_gather(ho_all, ho_send, ho_recv)
    out[...] = ho_all[...]
    for c in pending:
        c.wait_send()

    @pl.when(end)
    def _():
        for i in range(NP):
            near_copy(i, nrecv, nr_sem).wait_send()
            for c in m_copies(i):
                c.wait_send()

    @pl.when(mid)
    def _():
        for i in range(NP):
            near_copy(i, frecv, fr_sem).wait_send()
            far_copy(i).wait_send()


def local_layer(hidden, w_q, w_k, w_v, w_o, w_gate, w_up, w_down, norm_attn, norm_mlp, k_cache, v_cache, seq_lens, rope_cos, rope_sin):
    mib = 1 << 20

    def hbm(*arrays):
        return [pltpu.with_memory_space_constraint(a, pltpu.HBM) for a in arrays]

    def vmem(*arrays):
        return [pltpu.with_memory_space_constraint(a, pltpu.VMEM) for a in arrays]

    q, kn, vn, kc, vc = pl.pallas_call(
        qkv_kernel,
        out_shape=(pltpu.VMEM((RB, 8, HD), F32), pltpu.VMEM((RB, 8, HD), F32), pltpu.VMEM((RB, 8, HD), F32),
                   pltpu.VMEM((RB * SEQ2, HD), BF16), pltpu.VMEM((RB * SEQ2, HD), BF16)),
        in_specs=[ANY] * 9,
        out_specs=(VM,) * 5,
        scratch_shapes=[
            pltpu.VMEM((ROWS, W), BF16), pltpu.VMEM((W,), BF16), pltpu.VMEM((NH, W, HD), BF16),
            pltpu.VMEM((2 * W, HD), BF16), pltpu.VMEM((2 * W, HD), BF16), pltpu.VMEM((RB, HD // 2), F32), pltpu.VMEM((RB, HD // 2), F32),
            pltpu.VMEM((ROWS, PAY), F32), pltpu.VMEM((NZ - 1, RB, PAY), F32),
            DMA((7,)), DMA((2,)), DMA((3,)), DMA((3,))],
        compiler_params=pltpu.CompilerParams(collective_id=0, has_side_effects=True, vmem_limit_bytes=40 * mib),
        name='qkv',
    )(*hbm(hidden, norm_attn, w_q.transpose(1, 0, 2), w_k.reshape(2 * W, HD), w_v.reshape(2 * W, HD), rope_cos, rope_sin,
           k_cache.reshape(RB * SEQ2, HD), v_cache.reshape(RB * SEQ2, HD)))

    o, k_out, v_out, _, _ = pl.pallas_call(
        attn_kernel,
        out_shape=(pltpu.VMEM((RB, W), BF16), jax.ShapeDtypeStruct((RB * SEQ2, HD), BF16), jax.ShapeDtypeStruct((RB * SEQ2, HD), BF16),
                   pltpu.VMEM((RB * SEQ2, HD), BF16), pltpu.VMEM((RB * SEQ2, HD), BF16)),
        in_specs=[SM, VM, VM, VM, VM, VM],
        out_specs=(VM, ANY, ANY, VM, VM),
        scratch_shapes=[pltpu.VMEM((RB, 8, HD), F32), DMA((2, RB))],
        input_output_aliases={4: 3, 5: 4},
        compiler_params=pltpu.CompilerParams(vmem_limit_bytes=40 * mib),
        name='attn',
    )(seq_lens, *vmem(q, kn, vn, kc, vc))

    h_out = pl.pallas_call(
        tail_kernel,
        out_shape=jax.ShapeDtypeStruct((ROWS, W), BF16),
        in_specs=[VM] + [ANY] * 6,
        out_specs=VM,
        scratch_shapes=[
            pltpu.VMEM((NZ - 1, RB, W), BF16), pltpu.VMEM((ROWS, W), BF16), pltpu.VMEM((W,), BF16),
            pltpu.VMEM((W, W), BF16), pltpu.VMEM((W, FFL), BF16), pltpu.VMEM((W, FFL), BF16), pltpu.VMEM((FFL, W), BF16),
            pltpu.VMEM((ROWS, W), F32), pltpu.VMEM((NT - 1, RB, W), F32), pltpu.VMEM((ROWS, W), BF16),
            pltpu.VMEM((8, ROWS), F32), pltpu.VMEM((NZ - 1, 8, ROWS), F32),
            pltpu.VMEM((NP, ROWS, 2 * PC), F32), pltpu.VMEM((NP, ROWS, 2 * PC), F32), pltpu.VMEM((NP, ROWS, 2 * PC), F32),
            pltpu.VMEM((NP, ROWS, 2 * PC), F32), pltpu.VMEM((2 * NP, ROWS, PC), BF16),
            pltpu.VMEM((ROWS, W), F32), pltpu.VMEM((NT - 1, RB, W), F32), pltpu.VMEM((ROWS, W), BF16),
            DMA((6,)), DMA((3,)), DMA((3,)), DMA((3,)), DMA((3,)), DMA((3,)), DMA((3,)), DMA((3,)), DMA((3,)),
            DMA((NP,)), DMA((NP,)), DMA((NP,)), DMA((NP,)), DMA((3, NP)), DMA((2 * NP,)), DMA((3,)), DMA((3,)), DMA((3,)), DMA((3,))],
        compiler_params=pltpu.CompilerParams(collective_id=1, has_side_effects=True, vmem_limit_bytes=40 * mib),
        name='tail',
    )(*vmem(o), *hbm(hidden, norm_mlp, w_o.reshape(W, W), w_gate, w_up, w_down))
    shape = (RB, SEQ2 // 2, 2, HD)
    return h_out, k_out.reshape(shape), v_out.reshape(shape)


def solution(mesh):
    row_spec = P('dp', 'dm')
    cache_spec = P(('dp', 'dm'), None, 'tp', None)
    batch_spec = P(('dp', 'dm'))
    rope_spec = P(('dp', 'dm'), None)
    in_specs = (row_spec, P('dm', 'tp', None), P('dm', 'tp', None), P('dm', 'tp', None), P('tp', None, 'dm'), P('dm', 'tp'), P('dm', 'tp'), P('tp', 'dm'), P('dm'), P('dm'), cache_spec, cache_spec, batch_spec, rope_spec, rope_spec)
    return jax.shard_map(local_layer, mesh=mesh, in_specs=in_specs, out_specs=(row_spec, cache_spec, cache_spec), check_vma=False)
```

```python
import jax
import jax.numpy as jnp
from jax import lax
from jax.experimental import pallas as pl
from jax.experimental.pallas import tpu as pltpu
from jax.sharding import PartitionSpec as P

EPS = 1e-6
F32 = jnp.float32
BF16 = jnp.bfloat16
MESH = pl.DeviceIdType.MESH
ANY = pl.BlockSpec(memory_space=pl.ANY)
VM = pl.BlockSpec(memory_space=pltpu.VMEM)
SM = pl.BlockSpec(memory_space=pltpu.SMEM)
DMA = pltpu.SemaphoreType.DMA

NZ = 4
NT = 4
ROWS = 64
RB = 16
W = 768
HD = 128
NH = 6
GRP = 3
SEQ2 = 2048
QKV = (NH + 4) * HD
PAY = QKV + HD
FFL = 2048
NP = 8
PC = 128
NS = 2
SUB = ROWS // NS


def partners(i):
    return (3 - i, (i + 2) % 4, i + 1 - 2 * (i % 2))


def dot(a, b):
    return jnp.dot(a, b, preferred_element_type=F32)


def local_scale(x, width):
    ss = jnp.sum(x * x, axis=-1, keepdims=True)
    return ss, lax.rsqrt(ss / width + EPS)


def qkv_kernel(hid, gain, wq, wk, wv, cos, sin, kc, vc,
               q_o, k_o, v_o, kc_o, vc_o,
               h_s, g_s, wq_s, wk_s, wv_s, cos_s, sin_s, part, recv,
               in_sem, c_sem, send_sem, recv_sem):
    z = lax.axis_index('dm')
    peers = partners(z)
    ins = [pltpu.make_async_copy(s, d, in_sem.at[i]) for i, (s, d) in enumerate(
        ((hid, h_s), (gain, g_s), (wk, wk_s), (wv, wv_s), (wq, wq_s), (cos, cos_s), (sin, sin_s)))]
    for c in ins:
        c.start()
    caches = [pltpu.make_async_copy(kc, kc_o, c_sem.at[0]), pltpu.make_async_copy(vc, vc_o, c_sem.at[1])]
    for c in caches:
        c.start()
    barrier = pltpu.get_barrier_semaphore()
    for p in peers:
        pl.semaphore_signal(barrier, inc=1, device_id={'dm': p}, device_id_type=MESH)

    ins[0].wait()
    ins[1].wait()
    h = h_s[...].astype(F32)
    ss, scale = local_scale(h, W)
    part[:, QKV:PAY] = jnp.broadcast_to(ss, (ROWS, HD))
    x = (h * scale * g_s[...].astype(F32).reshape(1, W)).astype(BF16)
    rr = lax.broadcasted_iota(jnp.int32, (HD, 2 * HD), 0)
    cc = lax.broadcasted_iota(jnp.int32, (HD, 2 * HD), 1)
    spread = []
    for hd in range(2):
        sel = jnp.where(cc == 2 * rr + hd, 1.0, 0.0).astype(BF16)
        spread.append(jnp.concatenate(
            [dot(x[:, j * HD:(j + 1) * HD], sel).astype(BF16) for j in range(W // HD)], axis=1))
    xe = jnp.concatenate(spread, axis=0)
    ins[2].wait()
    kk = dot(xe, wk_s[...])
    ins[3].wait()
    vv = dot(xe, wv_s[...])
    for hd in range(2):
        part[:, (NH + hd) * HD:(NH + hd + 1) * HD] = kk[hd * ROWS:(hd + 1) * ROWS]
        part[:, (NH + 2 + hd) * HD:(NH + 3 + hd) * HD] = vv[hd * ROWS:(hd + 1) * ROWS]
    ins[4].wait()
    for hd in range(NH):
        part[:, hd * HD:(hd + 1) * HD] = dot(x, wq_s[hd])
    pl.semaphore_wait(barrier, NZ - 1)
    copies = []
    for k, p in enumerate(peers):
        c = pltpu.make_async_remote_copy(
            src_ref=part.at[pl.ds(pl.multiple_of(p * RB, RB), RB)], dst_ref=recv.at[k], send_sem=send_sem.at[k], recv_sem=recv_sem.at[k],
            device_id={'dm': p}, device_id_type=MESH)
        c.start()
        copies.append(c)
    ins[5].wait()
    ins[6].wait()
    own = part[pl.ds(pl.multiple_of(z * RB, RB), RB), :]
    for c in copies:
        c.wait_recv()
    parts = [own] + [recv[k] for k in range(NZ - 1)]
    stats = [t[:, QKV:PAY] for t in parts]
    glob = lax.rsqrt((stats[0] + stats[1] + stats[2] + stats[3]) / (NZ * W) + EPS)
    ratio = [glob * jnp.sqrt(s / W + EPS) for s in stats]

    def head(i):
        cols = slice(i * HD, (i + 1) * HD)
        return sum(t[:, cols] * r for t, r in zip(parts, ratio))

    cs = jnp.concatenate([cos_s[...], cos_s[...]], axis=1)
    sn = jnp.concatenate([-sin_s[...], sin_s[...]], axis=1)

    def rope(t):
        return (t * cs + pltpu.roll(t, HD // 2, 1) * sn).astype(BF16).astype(F32)

    for i in range(NH):
        q_o[:, i, :] = rope(head(i))
    for i in range(NH, 8):
        q_o[:, i, :] = jnp.zeros((RB, HD), F32)
    for hd in range(2):
        kn = rope(head(NH + hd))
        vn = head(NH + 2 + hd).astype(BF16).astype(F32)
        for r in range(hd, 8, 2):
            k_o[:, r, :] = kn
            v_o[:, r, :] = vn
    for c in copies:
        c.wait_send()
    for c in caches:
        c.wait()


def patch_kernel(lens, kn, vn, kc, vc, kc_a, vc_a):
    del kc, vc
    r16 = lax.broadcasted_iota(jnp.int32, (16, HD), 0)
    for b in range(RB):
        ln = lens[b]
        base = pl.multiple_of(b * SEQ2 + (ln // 8) * 16, 16)
        hit = (r16 // 2) == (ln % 8)
        for new, cache in ((kn, kc_a), (vn, vc_a)):
            fresh = jnp.concatenate([new[b], new[b]], axis=0)
            tile = cache[pl.ds(base, 16), :].astype(F32)
            cache[pl.ds(base, 16), :] = jnp.where(hit, fresh, tile).astype(BF16)


def tail_kernel(lens, q, kc, vc, hid, gain, w_o, w_g, w_u, w_d, out,
                o_s, o_mine, o_all, h_s, g_s, wo_s, wg_s, wu_s, wd_s, part, dd1, ys1, yr1, h1_all, st_send, st_recv,
                nsend, fsend, nrecv, frecv, m_all, part2, dd2, ys2, yr2, ho_all,
                w_sem, o_send, o_recv, ar1, ar2, st_ss, st_rs,
                ns_sem, fs_sem, nr_sem, fr_sem, m_send, m_recv):
    z = lax.axis_index('dm')
    t = lax.axis_index('tp')
    zp = partners(z)
    core = lax.rem(t, 2)
    twin, across = t + 1 - 2 * core, lax.rem(t + 2, 4)
    loads = [pltpu.make_async_copy(s, d, w_sem.at[i]) for i, (s, d) in enumerate(
        ((w_o, wo_s), (hid, h_s), (gain, g_s), (w_g, wg_s), (w_u, wu_s), (w_d, wd_s)))]
    for c in loads:
        c.start()
    barrier = pltpu.get_barrier_semaphore()
    for p in zp:
        pl.semaphore_signal(barrier, inc=1, device_id={'dm': p}, device_id_type=MESH)
    for p in (twin, across):
        pl.semaphore_signal(barrier, inc=1, device_id={'tp': p}, device_id_type=MESH)

    def remote(src, dst, ss, rs, dev):
        c = pltpu.make_async_remote_copy(src_ref=src, dst_ref=dst, send_sem=ss, recv_sem=rs, device_id=dev, device_id_type=MESH)
        c.start()
        return c

    def my(i):
        return pl.ds(pl.multiple_of(i * RB, RB), RB)

    pending = []
    row = lax.broadcasted_iota(jnp.int32, (16, SEQ2), 0)
    column = lax.broadcasted_iota(jnp.int32, (16, SEQ2), 1)
    same_head = (column % 2) == jnp.where(row % 8 < GRP, 0, 1)
    slot = jnp.where(same_head, column // 2, SEQ2)
    zero = jnp.zeros((8, HD), F32)
    row1 = lax.broadcasted_iota(jnp.int32, (16, 1), 0)
    cps = []
    for half in range(2):
        for b in range(8 * half, 8 * half + 8, 2):
            lhs = jnp.concatenate([jnp.concatenate([q[b], zero], axis=1),
                                   jnp.concatenate([zero, q[b + 1]], axis=1)], axis=0).astype(BF16)
            r0, r1 = pl.ds(b * SEQ2, SEQ2), pl.ds((b + 1) * SEQ2, SEQ2)
            kk = jnp.concatenate([kc[r0, :], kc[r1, :]], axis=1)
            s = lax.dot_general(lhs, kk, (((1,), (1,)), ((), ())), preferred_element_type=F32)
            ln = jnp.where(row1 < 8, lens[b], lens[b + 1])
            s = jnp.where(slot <= ln, s * (HD ** -0.5), -1e30)
            e = jnp.exp(s - jnp.max(s, axis=1, keepdims=True))
            pr = (e * (1.0 / jnp.sum(e, axis=1, keepdims=True))).astype(BF16)
            vv = jnp.concatenate([vc[r0, :], vc[r1, :]], axis=1)
            oo = dot(pr, vv)
            o_s[b] = oo[:8, :HD]
            o_s[b + 1] = oo[8:, HD:]
        rows = pl.ds(8 * half, 8)
        for hd in range(NH):
            o_mine[rows, hd * HD:(hd + 1) * HD] = o_s[rows, hd, :].astype(BF16)
        if half == 0:
            pl.semaphore_wait(barrier, 5)
        cps.append([remote(o_mine.at[rows], o_all.at[k, rows], o_send.at[k, half], o_recv.at[k, half], {'dm': p})
                    for k, p in enumerate(zp)])
    loads[0].wait()
    part[my(z), :] = dot(o_mine[...], wo_s[...])
    for k in (2, 1, 0):
        for half in range(2):
            cps[half][k].wait_recv()
            pending.append(cps[half][k])
        part[my(zp[k]), :] = dot(o_all[k], wo_s[...])

    def tp_sum(buf, base, dd, ys, yr, res, sems):
        def rws(c, i):
            return pl.ds(pl.multiple_of(c * 2 * RB + i * RB, RB), RB)
        first = [remote(buf.at[rws(1 - core, i)], dd.at[i], sems.at[0, i], sems.at[1, i], {'tp': twin}) for i in range(2)]
        second, third = [], []
        for i in range(2):
            first[i].wait_recv()
            ys[i] = buf[rws(core, i), :] + dd[i]
            second.append(remote(ys.at[i], yr.at[i], sems.at[2, i], sems.at[3, i], {'tp': across}))
        for i in range(2):
            second[i].wait_recv()
            tot = ys[i] + yr[i]
            res[rws(core, i), :] = (base[rws(core, i), :].astype(F32) + tot.astype(BF16).astype(F32)).astype(BF16)
            third.append(remote(res.at[rws(core, i)], res.at[rws(core, i)], sems.at[4, i], sems.at[5, i], {'tp': twin}))
        for c in third:
            c.wait_recv()
        pending.extend(first + second + third)

    loads[1].wait()
    tp_sum(part, h_s, dd1, ys1, yr1, h1_all, ar1)
    hf = h1_all[...].astype(F32)
    ss, scale = local_scale(hf, W)
    ssb = jnp.broadcast_to(ss, (ROWS, HD))
    st_send[...] = jnp.transpose(ssb)[:8, :]
    scp = [remote(st_send, st_recv.at[k], st_ss.at[k], st_rs.at[k], {'dm': p}) for k, p in enumerate(zp)]
    pending += scp
    loads[2].wait()
    x2 = (hf * scale * g_s[...].astype(F32).reshape(1, W)).astype(BF16)
    loads[3].wait()
    loads[4].wait()

    nd = z // 2
    end = (z % 3) == 0
    mid = jnp.logical_not(end)
    step = 1 - 2 * nd
    near_dst, far_dst = z + step, z - step
    near_ok, far_ok = {'dm': lax.rem(near_dst + NZ, NZ)}, {'dm': lax.rem(far_dst + NZ, NZ)}

    def piece(c):
        cols = pl.ds(pl.multiple_of(c * PC, PC), PC)
        return dot(x2, jnp.concatenate([wg_s[:, cols], wu_s[:, cols]], axis=1))

    def sub(h):
        return pl.ds(h * SUB, SUB)

    def near_copy(i, h, dst, rsem):
        return pltpu.make_async_remote_copy(src_ref=nsend.at[i, sub(h)], dst_ref=dst.at[i, sub(h)], send_sem=ns_sem.at[i, h],
                                            recv_sem=rsem.at[i, h], device_id=near_ok, device_id_type=MESH)

    def far_copy(i, h):
        return pltpu.make_async_remote_copy(src_ref=fsend.at[i, sub(h)], dst_ref=frecv.at[i, sub(h)], send_sem=fs_sem.at[i, h],
                                            recv_sem=fr_sem.at[i, h], device_id=far_ok, device_id_type=MESH)

    def m_copies(i):
        cb = (1 - nd) * NP + i
        return [pltpu.make_async_remote_copy(src_ref=m_all.at[cb], dst_ref=m_all.at[cb], send_sem=m_send.at[k, i], recv_sem=m_recv.at[cb],
                                             device_id={'dm': p}, device_id_type=MESH) for k, p in enumerate(zp)]

    @pl.when(end)
    def _():
        for i in range(NP):
            nsend[i] = piece(nd * NP + i)
            for h in range(NS):
                near_copy(i, h, nrecv, nr_sem).start()

    for c in scp:
        c.wait_recv()

    def col(row8):
        return jnp.transpose(jnp.broadcast_to(row8[0:1, :], (HD, ROWS)))

    sts = [col(st_recv[k]) for k in range(NZ - 1)]
    glob = lax.rsqrt((ssb + sts[0] + sts[1] + sts[2]) / (NZ * W) + EPS)
    r_me = glob * jnp.sqrt(ssb / W + EPS)
    r_end = glob * jnp.sqrt(sts[2] / W + EPS)
    r_me2 = jnp.concatenate([r_me, r_me], axis=1)
    r_end2 = jnp.concatenate([r_end, r_end], axis=1)

    @pl.when(mid)
    def _():
        def near(i):
            mine = piece(nd * NP + i) * r_me2
            for h in range(NS):
                near_copy(i, h, nrecv, nr_sem).wait_recv()
                r = slice(h * SUB, (h + 1) * SUB)
                nsend[i, r] = nrecv[i, r] * r_end2[r] + mine[r]
                near_copy(i, h, frecv, fr_sem).start()

        def far(i):
            mine = piece((1 - nd) * NP + i) * r_me2
            for h in range(NS):
                far_copy(i, h).wait_recv()
                r = slice(h * SUB, (h + 1) * SUB)
                fsend[i, r] = frecv[i, r] + mine[r]
                far_copy(i, h).start()

        for i in range(NP + 2):
            if i < NP:
                near(i)
            if i >= 2:
                far(i - 2)

    @pl.when(end)
    def _():
        for i in range(NP):
            mine = piece((1 - nd) * NP + i) * r_me2
            for h in range(NS):
                far_copy(i, h).wait_recv()
            tot = frecv[i] + mine
            gate, up = tot[:, :PC], tot[:, PC:]
            m_all[(1 - nd) * NP + i] = (gate * (1.0 / (1.0 + jnp.exp(-gate))) * up).astype(BF16)
            for c in m_copies(i):
                c.start()

    def m_wait(cb, i):
        pltpu.make_async_remote_copy(src_ref=m_all.at[cb], dst_ref=m_all.at[cb], send_sem=m_send.at[0, i], recv_sem=m_recv.at[cb],
                                     device_id={'dm': zp[0]}, device_id_type=MESH).wait_recv()

    loads[5].wait()
    for i in range(NP):
        m_wait(nd * NP + i, i)

        @pl.when(mid)
        def _():
            m_wait((1 - nd) * NP + i, i)

    acc = None
    for j in range(NP):
        d = dot(jnp.concatenate([m_all[2 * j], m_all[2 * j + 1]], axis=1), wd_s[2 * j * PC:2 * (j + 1) * PC, :])
        acc = d if acc is None else acc + d
    part2[...] = acc
    tp_sum(part2, h1_all, dd2, ys2, yr2, ho_all, ar2)
    out[...] = ho_all[...]
    for c in pending:
        c.wait_send()

    @pl.when(end)
    def _():
        for i in range(NP):
            for h in range(NS):
                near_copy(i, h, nrecv, nr_sem).wait_send()
            for c in m_copies(i):
                c.wait_send()

    @pl.when(mid)
    def _():
        for i in range(NP):
            for h in range(NS):
                near_copy(i, h, frecv, fr_sem).wait_send()
                far_copy(i, h).wait_send()


def local_layer(hidden, w_q, w_k, w_v, w_o, w_gate, w_up, w_down, norm_attn, norm_mlp, k_cache, v_cache, seq_lens, rope_cos, rope_sin):
    mib = 1 << 20

    def hbm(*arrays):
        return [pltpu.with_memory_space_constraint(a, pltpu.HBM) for a in arrays]

    def vmem(*arrays):
        return [pltpu.with_memory_space_constraint(a, pltpu.VMEM) for a in arrays]

    q, kn, vn, kc, vc = pl.pallas_call(
        qkv_kernel,
        out_shape=(pltpu.VMEM((RB, 8, HD), F32), pltpu.VMEM((RB, 8, HD), F32), pltpu.VMEM((RB, 8, HD), F32),
                   pltpu.VMEM((RB * SEQ2, HD), BF16), pltpu.VMEM((RB * SEQ2, HD), BF16)),
        in_specs=[ANY] * 9,
        out_specs=(VM,) * 5,
        scratch_shapes=[
            pltpu.VMEM((ROWS, W), BF16), pltpu.VMEM((W,), BF16), pltpu.VMEM((NH, W, HD), BF16),
            pltpu.VMEM((2 * W, HD), BF16), pltpu.VMEM((2 * W, HD), BF16), pltpu.VMEM((RB, HD // 2), F32), pltpu.VMEM((RB, HD // 2), F32),
            pltpu.VMEM((ROWS, PAY), F32), pltpu.VMEM((NZ - 1, RB, PAY), F32),
            DMA((7,)), DMA((2,)), DMA((3,)), DMA((3,))],
        compiler_params=pltpu.CompilerParams(collective_id=0, has_side_effects=True, vmem_limit_bytes=40 * mib),
        name='qkv',
    )(*hbm(hidden, norm_attn, w_q.transpose(1, 0, 2), w_k.reshape(2 * W, HD), w_v.reshape(2 * W, HD), rope_cos, rope_sin,
           k_cache.reshape(RB * SEQ2, HD), v_cache.reshape(RB * SEQ2, HD)))

    kc, vc = pl.pallas_call(
        patch_kernel,
        out_shape=(pltpu.VMEM((RB * SEQ2, HD), BF16), pltpu.VMEM((RB * SEQ2, HD), BF16)),
        in_specs=[SM, VM, VM, VM, VM],
        out_specs=(VM, VM),
        input_output_aliases={3: 0, 4: 1},
        compiler_params=pltpu.CompilerParams(vmem_limit_bytes=4 * mib),
        name='patch',
    )(seq_lens, *vmem(kn, vn, kc, vc))

    h_out = pl.pallas_call(
        tail_kernel,
        out_shape=jax.ShapeDtypeStruct((ROWS, W), BF16),
        in_specs=[SM, VM, VM, VM] + [ANY] * 6,
        out_specs=VM,
        scratch_shapes=[
            pltpu.VMEM((RB, 8, HD), F32), pltpu.VMEM((RB, W), BF16),
            pltpu.VMEM((NZ - 1, RB, W), BF16), pltpu.VMEM((ROWS, W), BF16), pltpu.VMEM((W,), BF16),
            pltpu.VMEM((W, W), BF16), pltpu.VMEM((W, FFL), BF16), pltpu.VMEM((W, FFL), BF16), pltpu.VMEM((FFL, W), BF16),
            pltpu.VMEM((ROWS, W), F32), pltpu.VMEM((2, RB, W), F32), pltpu.VMEM((2, RB, W), F32), pltpu.VMEM((2, RB, W), F32),
            pltpu.VMEM((ROWS, W), BF16),
            pltpu.VMEM((8, ROWS), F32), pltpu.VMEM((NZ - 1, 8, ROWS), F32),
            pltpu.VMEM((NP, ROWS, 2 * PC), F32), pltpu.VMEM((NP, ROWS, 2 * PC), F32), pltpu.VMEM((NP, ROWS, 2 * PC), F32),
            pltpu.VMEM((NP, ROWS, 2 * PC), F32), pltpu.VMEM((2 * NP, ROWS, PC), BF16),
            pltpu.VMEM((ROWS, W), F32), pltpu.VMEM((2, RB, W), F32), pltpu.VMEM((2, RB, W), F32), pltpu.VMEM((2, RB, W), F32),
            pltpu.VMEM((ROWS, W), BF16),
            DMA((6,)), DMA((3, 2)), DMA((3, 2)), DMA((6, 2)), DMA((6, 2)), DMA((3,)), DMA((3,)),
            DMA((NP, NS)), DMA((NP, NS)), DMA((NP, NS)), DMA((NP, NS)), DMA((3, NP)), DMA((2 * NP,))],
        compiler_params=pltpu.CompilerParams(collective_id=1, has_side_effects=True, vmem_limit_bytes=40 * mib),
        cost_estimate=pl.CostEstimate(flops=40_000_000_000, bytes_accessed=30_000_000, transcendentals=0),
        name='tail',
    )(seq_lens, *vmem(q, kc, vc), *hbm(hidden, norm_mlp, w_o.reshape(W, W), w_gate, w_up, w_down))
    k_out, v_out = kc, vc
    shape = (RB, SEQ2 // 2, 2, HD)
    return h_out, k_out.reshape(shape), v_out.reshape(shape)


def solution(mesh):
    row_spec = P('dp', 'dm')
    cache_spec = P(('dp', 'dm'), None, 'tp', None)
    batch_spec = P(('dp', 'dm'))
    rope_spec = P(('dp', 'dm'), None)
    in_specs = (row_spec, P('dm', 'tp', None), P('dm', 'tp', None), P('dm', 'tp', None), P('tp', None, 'dm'), P('dm', 'tp'), P('dm', 'tp'), P('tp', 'dm'), P('dm'), P('dm'), cache_spec, cache_spec, batch_spec, rope_spec, rope_spec)
    return jax.shard_map(local_layer, mesh=mesh, in_specs=in_specs, out_specs=(row_spec, cache_spec, cache_spec), check_vma=False)
```

```python
import jax
import jax.numpy as jnp
from jax import lax
from jax.experimental import pallas as pl
from jax.experimental.pallas import tpu as pltpu
from jax.sharding import PartitionSpec as P

EPS = 1e-6
F32 = jnp.float32
BF16 = jnp.bfloat16
MESH = pl.DeviceIdType.MESH
ANY = pl.BlockSpec(memory_space=pl.ANY)
VM = pl.BlockSpec(memory_space=pltpu.VMEM)
SM = pl.BlockSpec(memory_space=pltpu.SMEM)
DMA = pltpu.SemaphoreType.DMA

NZ = 4
NT = 4
ROWS = 64
RB = 16
W = 768
HD = 128
NH = 6
GRP = 3
SEQ2 = 2048
QKV = (NH + 4) * HD
PAY = QKV + HD
FFL = 2048
NP = 8
PC = 128
NS = 2
SUB = ROWS // NS


def partners(i):
    return (3 - i, (i + 2) % 4, i + 1 - 2 * (i % 2))


def dot(a, b):
    return jnp.dot(a, b, preferred_element_type=F32)


def local_scale(x, width):
    ss = jnp.sum(x * x, axis=-1, keepdims=True)
    return ss, lax.rsqrt(ss / width + EPS)


def qkv_kernel(hid, gain, wq, wk, wv, cos, sin, kc, vc,
               q_o, k_o, v_o, kc_o, vc_o,
               h_s, g_s, wq_s, wk_s, wv_s, cos_s, sin_s, part, recv,
               in_sem, c_sem, send_sem, recv_sem):
    z = lax.axis_index('dm')
    peers = partners(z)
    ins = [pltpu.make_async_copy(s, d, in_sem.at[i]) for i, (s, d) in enumerate(
        ((hid, h_s), (gain, g_s), (wk, wk_s), (wv, wv_s), (wq, wq_s), (cos, cos_s), (sin, sin_s)))]
    for c in ins:
        c.start()
    caches = [pltpu.make_async_copy(kc, kc_o, c_sem.at[0]), pltpu.make_async_copy(vc, vc_o, c_sem.at[1])]
    for c in caches:
        c.start()
    barrier = pltpu.get_barrier_semaphore()
    for p in peers:
        pl.semaphore_signal(barrier, inc=1, device_id={'dm': p}, device_id_type=MESH)

    ins[0].wait()
    ins[1].wait()
    h = h_s[...].astype(F32)
    ss, scale = local_scale(h, W)
    part[:, QKV:PAY] = jnp.broadcast_to(ss, (ROWS, HD))
    x = (h * scale * g_s[...].astype(F32).reshape(1, W)).astype(BF16)
    rr = lax.broadcasted_iota(jnp.int32, (HD, 2 * HD), 0)
    cc = lax.broadcasted_iota(jnp.int32, (HD, 2 * HD), 1)
    spread = []
    for hd in range(2):
        sel = jnp.where(cc == 2 * rr + hd, 1.0, 0.0).astype(BF16)
        spread.append(jnp.concatenate(
            [dot(x[:, j * HD:(j + 1) * HD], sel).astype(BF16) for j in range(W // HD)], axis=1))
    xe = jnp.concatenate(spread, axis=0)
    ins[2].wait()
    kk = dot(xe, wk_s[...])
    ins[3].wait()
    vv = dot(xe, wv_s[...])
    for hd in range(2):
        part[:, (NH + hd) * HD:(NH + hd + 1) * HD] = kk[hd * ROWS:(hd + 1) * ROWS]
        part[:, (NH + 2 + hd) * HD:(NH + 3 + hd) * HD] = vv[hd * ROWS:(hd + 1) * ROWS]
    ins[4].wait()
    for hd in range(NH):
        part[:, hd * HD:(hd + 1) * HD] = dot(x, wq_s[hd])
    pl.semaphore_wait(barrier, NZ - 1)
    copies = []
    for k, p in enumerate(peers):
        c = pltpu.make_async_remote_copy(
            src_ref=part.at[pl.ds(pl.multiple_of(p * RB, RB), RB)], dst_ref=recv.at[k], send_sem=send_sem.at[k], recv_sem=recv_sem.at[k],
            device_id={'dm': p}, device_id_type=MESH)
        c.start()
        copies.append(c)
    ins[5].wait()
    ins[6].wait()
    own = part[pl.ds(pl.multiple_of(z * RB, RB), RB), :]
    for c in copies:
        c.wait_recv()
    parts = [own] + [recv[k] for k in range(NZ - 1)]
    stats = [t[:, QKV:PAY] for t in parts]
    glob = lax.rsqrt((stats[0] + stats[1] + stats[2] + stats[3]) / (NZ * W) + EPS)
    ratio = [glob * jnp.sqrt(s / W + EPS) for s in stats]

    def head(i):
        cols = slice(i * HD, (i + 1) * HD)
        return sum(t[:, cols] * r for t, r in zip(parts, ratio))

    cs = jnp.concatenate([cos_s[...], cos_s[...]], axis=1)
    sn = jnp.concatenate([-sin_s[...], sin_s[...]], axis=1)

    def rope(t):
        return (t * cs + pltpu.roll(t, HD // 2, 1) * sn).astype(BF16).astype(F32)

    for i in range(NH):
        q_o[:, i, :] = rope(head(i))
    for i in range(NH, 8):
        q_o[:, i, :] = jnp.zeros((RB, HD), F32)
    for hd in range(2):
        kn = rope(head(NH + hd))
        vn = head(NH + 2 + hd).astype(BF16).astype(F32)
        for r in range(hd, 8, 2):
            k_o[:, r, :] = kn
            v_o[:, r, :] = vn
    for c in copies:
        c.wait_send()
    for c in caches:
        c.wait()


def attn_kernel(lens, q, kn, vn, kc, vc, o, k_out, v_out, kc_a, vc_a, o_s, sem):
    del kc, vc
    r16 = lax.broadcasted_iota(jnp.int32, (16, HD), 0)
    writes = []
    for b in range(RB):
        ln = lens[b]
        base = pl.multiple_of(b * SEQ2 + (ln // 8) * 16, 16)
        hit = (r16 // 2) == (ln % 8)
        for j, (new, cache, out) in enumerate(((kn, kc_a, k_out), (vn, vc_a, v_out))):
            fresh = jnp.concatenate([new[b], new[b]], axis=0)
            tile = cache[pl.ds(base, 16), :].astype(F32)
            cache[pl.ds(base, 16), :] = jnp.where(hit, fresh, tile).astype(BF16)
            rows = pl.ds(b * SEQ2, SEQ2)
            w = pltpu.make_async_copy(cache.at[rows], out.at[rows], sem.at[j, b])
            w.start()
            writes.append(w)
    row = lax.broadcasted_iota(jnp.int32, (16, SEQ2), 0)
    col = lax.broadcasted_iota(jnp.int32, (16, SEQ2), 1)
    same_head = (col % 2) == jnp.where(row % 8 < GRP, 0, 1)
    slot = jnp.where(same_head, col // 2, SEQ2)
    zero = jnp.zeros((8, HD), F32)
    row1 = lax.broadcasted_iota(jnp.int32, (16, 1), 0)
    for b in range(0, RB, 2):
        lhs = jnp.concatenate([jnp.concatenate([q[b], zero], axis=1),
                               jnp.concatenate([zero, q[b + 1]], axis=1)], axis=0).astype(BF16)
        r0, r1 = pl.ds(b * SEQ2, SEQ2), pl.ds((b + 1) * SEQ2, SEQ2)
        kk = jnp.concatenate([kc_a[r0, :], kc_a[r1, :]], axis=1)
        s = lax.dot_general(lhs, kk, (((1,), (1,)), ((), ())), preferred_element_type=F32)
        ln = jnp.where(row1 < 8, lens[b], lens[b + 1])
        s = jnp.where(slot <= ln, s * (HD ** -0.5), -1e30)
        e = jnp.exp(s - jnp.max(s, axis=1, keepdims=True))
        pr = (e * (1.0 / jnp.sum(e, axis=1, keepdims=True))).astype(BF16)
        vv = jnp.concatenate([vc_a[r0, :], vc_a[r1, :]], axis=1)
        oo = dot(pr, vv)
        o_s[b] = oo[:8, :HD]
        o_s[b + 1] = oo[8:, HD:]
    for hd in range(NH):
        o[:, hd * HD:(hd + 1) * HD] = o_s[:, hd, :].astype(BF16)
    for w in writes:
        w.wait()


def tail_kernel(o, hid, gain, w_o, w_g, w_u, w_d, out,
                o_all, h_s, g_s, wo_s, wg_s, wu_s, wd_s, part, dd1, ys1, yr1, h1_all, st_send, st_recv,
                nsend, fsend, nrecv, frecv, m_all, part2, dd2, ys2, yr2, ho_all,
                w_sem, o_send, o_recv, ar1, ar2, st_ss, st_rs,
                ns_sem, fs_sem, nr_sem, fr_sem, m_send, m_recv):
    z = lax.axis_index('dm')
    t = lax.axis_index('tp')
    zp = partners(z)
    core = lax.rem(t, 2)
    twin, across = t + 1 - 2 * core, lax.rem(t + 2, 4)
    loads = [pltpu.make_async_copy(s, d, w_sem.at[i]) for i, (s, d) in enumerate(
        ((w_o, wo_s), (hid, h_s), (gain, g_s), (w_g, wg_s), (w_u, wu_s), (w_d, wd_s)))]
    for c in loads:
        c.start()
    barrier = pltpu.get_barrier_semaphore()
    for p in zp:
        pl.semaphore_signal(barrier, inc=1, device_id={'dm': p}, device_id_type=MESH)
    for p in (twin, across):
        pl.semaphore_signal(barrier, inc=1, device_id={'tp': p}, device_id_type=MESH)

    def remote(src, dst, ss, rs, dev):
        c = pltpu.make_async_remote_copy(src_ref=src, dst_ref=dst, send_sem=ss, recv_sem=rs, device_id=dev, device_id_type=MESH)
        c.start()
        return c

    def my(i):
        return pl.ds(pl.multiple_of(i * RB, RB), RB)

    pending = []
    pl.semaphore_wait(barrier, 5)
    cps = [remote(o, o_all.at[k], o_send.at[k], o_recv.at[k], {'dm': p}) for k, p in enumerate(zp)]
    pending += cps
    loads[0].wait()
    part[my(z), :] = dot(o[...], wo_s[...])
    for k in (2, 1, 0):
        cps[k].wait_recv()
        part[my(zp[k]), :] = dot(o_all[k], wo_s[...])

    def tp_sum(buf, base, dd, ys, yr, res, sems):
        def rws(c, i):
            return pl.ds(pl.multiple_of(c * 2 * RB + i * RB, RB), RB)
        first = [remote(buf.at[rws(1 - core, i)], dd.at[i], sems.at[0, i], sems.at[1, i], {'tp': twin}) for i in range(2)]
        second, third = [], []
        for i in range(2):
            first[i].wait_recv()
            ys[i] = buf[rws(core, i), :] + dd[i]
            second.append(remote(ys.at[i], yr.at[i], sems.at[2, i], sems.at[3, i], {'tp': across}))
        for i in range(2):
            second[i].wait_recv()
            tot = ys[i] + yr[i]
            res[rws(core, i), :] = (base[rws(core, i), :].astype(F32) + tot.astype(BF16).astype(F32)).astype(BF16)
            third.append(remote(res.at[rws(core, i)], res.at[rws(core, i)], sems.at[4, i], sems.at[5, i], {'tp': twin}))
        for c in third:
            c.wait_recv()
        pending.extend(first + second + third)

    loads[1].wait()
    tp_sum(part, h_s, dd1, ys1, yr1, h1_all, ar1)
    hf = h1_all[...].astype(F32)
    ss, scale = local_scale(hf, W)
    ssb = jnp.broadcast_to(ss, (ROWS, HD))
    st_send[...] = jnp.transpose(ssb)[:8, :]
    scp = [remote(st_send, st_recv.at[k], st_ss.at[k], st_rs.at[k], {'dm': p}) for k, p in enumerate(zp)]
    pending += scp
    loads[2].wait()
    x2 = (hf * scale * g_s[...].astype(F32).reshape(1, W)).astype(BF16)
    loads[3].wait()
    loads[4].wait()

    nd = z // 2
    end = (z % 3) == 0
    mid = jnp.logical_not(end)
    step = 1 - 2 * nd
    near_dst, far_dst = z + step, z - step
    near_ok, far_ok = {'dm': lax.rem(near_dst + NZ, NZ)}, {'dm': lax.rem(far_dst + NZ, NZ)}

    def piece(c):
        cols = pl.ds(pl.multiple_of(c * PC, PC), PC)
        return dot(x2, jnp.concatenate([wg_s[:, cols], wu_s[:, cols]], axis=1))

    def sub(h):
        return pl.ds(h * SUB, SUB)

    def near_copy(i, h, dst, rsem):
        return pltpu.make_async_remote_copy(src_ref=nsend.at[i, sub(h)], dst_ref=dst.at[i, sub(h)], send_sem=ns_sem.at[i, h],
                                            recv_sem=rsem.at[i, h], device_id=near_ok, device_id_type=MESH)

    def far_copy(i, h):
        return pltpu.make_async_remote_copy(src_ref=fsend.at[i, sub(h)], dst_ref=frecv.at[i, sub(h)], send_sem=fs_sem.at[i, h],
                                            recv_sem=fr_sem.at[i, h], device_id=far_ok, device_id_type=MESH)

    def m_copies(i):
        cb = (1 - nd) * NP + i
        return [pltpu.make_async_remote_copy(src_ref=m_all.at[cb], dst_ref=m_all.at[cb], send_sem=m_send.at[k, i], recv_sem=m_recv.at[cb],
                                             device_id={'dm': p}, device_id_type=MESH) for k, p in enumerate(zp)]

    @pl.when(end)
    def _():
        for i in range(NP):
            nsend[i] = piece(nd * NP + i)
            for h in range(NS):
                near_copy(i, h, nrecv, nr_sem).start()

    for c in scp:
        c.wait_recv()

    def col(row8):
        return jnp.transpose(jnp.broadcast_to(row8[0:1, :], (HD, ROWS)))

    sts = [col(st_recv[k]) for k in range(NZ - 1)]
    glob = lax.rsqrt((ssb + sts[0] + sts[1] + sts[2]) / (NZ * W) + EPS)
    r_me = glob * jnp.sqrt(ssb / W + EPS)
    r_end = glob * jnp.sqrt(sts[2] / W + EPS)
    r_me2 = jnp.concatenate([r_me, r_me], axis=1)
    r_end2 = jnp.concatenate([r_end, r_end], axis=1)

    @pl.when(mid)
    def _():
        def near(i):
            mine = piece(nd * NP + i) * r_me2
            for h in range(NS):
                near_copy(i, h, nrecv, nr_sem).wait_recv()
                r = slice(h * SUB, (h + 1) * SUB)
                nsend[i, r] = nrecv[i, r] * r_end2[r] + mine[r]
                near_copy(i, h, frecv, fr_sem).start()

        def far(i):
            mine = piece((1 - nd) * NP + i) * r_me2
            for h in range(NS):
                far_copy(i, h).wait_recv()
                r = slice(h * SUB, (h + 1) * SUB)
                fsend[i, r] = frecv[i, r] + mine[r]
                far_copy(i, h).start()

        for i in range(NP + 2):
            if i < NP:
                near(i)
            if i >= 2:
                far(i - 2)

    @pl.when(end)
    def _():
        for i in range(NP):
            mine = piece((1 - nd) * NP + i) * r_me2
            for h in range(NS):
                far_copy(i, h).wait_recv()
            tot = frecv[i] + mine
            gate, up = tot[:, :PC], tot[:, PC:]
            m_all[(1 - nd) * NP + i] = (gate * (1.0 / (1.0 + jnp.exp(-gate))) * up).astype(BF16)
            for c in m_copies(i):
                c.start()

    def m_wait(cb, i):
        pltpu.make_async_remote_copy(src_ref=m_all.at[cb], dst_ref=m_all.at[cb], send_sem=m_send.at[0, i], recv_sem=m_recv.at[cb],
                                     device_id={'dm': zp[0]}, device_id_type=MESH).wait_recv()

    loads[5].wait()
    for i in range(NP):
        m_wait(nd * NP + i, i)

        @pl.when(mid)
        def _():
            m_wait((1 - nd) * NP + i, i)

    acc = None
    for j in range(NP):
        d = dot(jnp.concatenate([m_all[2 * j], m_all[2 * j + 1]], axis=1), wd_s[2 * j * PC:2 * (j + 1) * PC, :])
        acc = d if acc is None else acc + d
    part2[...] = acc
    tp_sum(part2, h1_all, dd2, ys2, yr2, ho_all, ar2)
    out[...] = ho_all[...]
    for c in pending:
        c.wait_send()

    @pl.when(end)
    def _():
        for i in range(NP):
            for h in range(NS):
                near_copy(i, h, nrecv, nr_sem).wait_send()
            for c in m_copies(i):
                c.wait_send()

    @pl.when(mid)
    def _():
        for i in range(NP):
            for h in range(NS):
                near_copy(i, h, frecv, fr_sem).wait_send()
                far_copy(i, h).wait_send()


def local_layer(hidden, w_q, w_k, w_v, w_o, w_gate, w_up, w_down, norm_attn, norm_mlp, k_cache, v_cache, seq_lens, rope_cos, rope_sin):
    mib = 1 << 20

    def hbm(*arrays):
        return [pltpu.with_memory_space_constraint(a, pltpu.HBM) for a in arrays]

    def vmem(*arrays):
        return [pltpu.with_memory_space_constraint(a, pltpu.VMEM) for a in arrays]

    q, kn, vn, kc, vc = pl.pallas_call(
        qkv_kernel,
        out_shape=(pltpu.VMEM((RB, 8, HD), F32), pltpu.VMEM((RB, 8, HD), F32), pltpu.VMEM((RB, 8, HD), F32),
                   pltpu.VMEM((RB * SEQ2, HD), BF16), pltpu.VMEM((RB * SEQ2, HD), BF16)),
        in_specs=[ANY] * 9,
        out_specs=(VM,) * 5,
        scratch_shapes=[
            pltpu.VMEM((ROWS, W), BF16), pltpu.VMEM((W,), BF16), pltpu.VMEM((NH, W, HD), BF16),
            pltpu.VMEM((2 * W, HD), BF16), pltpu.VMEM((2 * W, HD), BF16), pltpu.VMEM((RB, HD // 2), F32), pltpu.VMEM((RB, HD // 2), F32),
            pltpu.VMEM((ROWS, PAY), F32), pltpu.VMEM((NZ - 1, RB, PAY), F32),
            DMA((7,)), DMA((2,)), DMA((3,)), DMA((3,))],
        compiler_params=pltpu.CompilerParams(collective_id=0, has_side_effects=True, vmem_limit_bytes=40 * mib),
        name='qkv',
    )(*hbm(hidden, norm_attn, w_q.transpose(1, 0, 2), w_k.reshape(2 * W, HD), w_v.reshape(2 * W, HD), rope_cos, rope_sin,
           k_cache.reshape(RB * SEQ2, HD), v_cache.reshape(RB * SEQ2, HD)))

    o, k_out, v_out, _, _ = pl.pallas_call(
        attn_kernel,
        out_shape=(pltpu.VMEM((RB, W), BF16), jax.ShapeDtypeStruct((RB * SEQ2, HD), BF16), jax.ShapeDtypeStruct((RB * SEQ2, HD), BF16),
                   pltpu.VMEM((RB * SEQ2, HD), BF16), pltpu.VMEM((RB * SEQ2, HD), BF16)),
        in_specs=[SM, VM, VM, VM, VM, VM],
        out_specs=(VM, ANY, ANY, VM, VM),
        scratch_shapes=[pltpu.VMEM((RB, 8, HD), F32), DMA((2, RB))],
        input_output_aliases={4: 3, 5: 4},
        compiler_params=pltpu.CompilerParams(vmem_limit_bytes=40 * mib),
        name='attn',
    )(seq_lens, *vmem(q, kn, vn, kc, vc))

    h_out = pl.pallas_call(
        tail_kernel,
        out_shape=jax.ShapeDtypeStruct((ROWS, W), BF16),
        in_specs=[VM] + [ANY] * 6,
        out_specs=VM,
        scratch_shapes=[
            pltpu.VMEM((NZ - 1, RB, W), BF16), pltpu.VMEM((ROWS, W), BF16), pltpu.VMEM((W,), BF16),
            pltpu.VMEM((W, W), BF16), pltpu.VMEM((W, FFL), BF16), pltpu.VMEM((W, FFL), BF16), pltpu.VMEM((FFL, W), BF16),
            pltpu.VMEM((ROWS, W), F32), pltpu.VMEM((2, RB, W), F32), pltpu.VMEM((2, RB, W), F32), pltpu.VMEM((2, RB, W), F32),
            pltpu.VMEM((ROWS, W), BF16),
            pltpu.VMEM((8, ROWS), F32), pltpu.VMEM((NZ - 1, 8, ROWS), F32),
            pltpu.VMEM((NP, ROWS, 2 * PC), F32), pltpu.VMEM((NP, ROWS, 2 * PC), F32), pltpu.VMEM((NP, ROWS, 2 * PC), F32),
            pltpu.VMEM((NP, ROWS, 2 * PC), F32), pltpu.VMEM((2 * NP, ROWS, PC), BF16),
            pltpu.VMEM((ROWS, W), F32), pltpu.VMEM((2, RB, W), F32), pltpu.VMEM((2, RB, W), F32), pltpu.VMEM((2, RB, W), F32),
            pltpu.VMEM((ROWS, W), BF16),
            DMA((6,)), DMA((3,)), DMA((3,)), DMA((6, 2)), DMA((6, 2)), DMA((3,)), DMA((3,)),
            DMA((NP, NS)), DMA((NP, NS)), DMA((NP, NS)), DMA((NP, NS)), DMA((3, NP)), DMA((2 * NP,))],
        compiler_params=pltpu.CompilerParams(collective_id=1, has_side_effects=True, vmem_limit_bytes=40 * mib),
        name='tail',
    )(*vmem(o), *hbm(hidden, norm_mlp, w_o.reshape(W, W), w_gate, w_up, w_down))
    shape = (RB, SEQ2 // 2, 2, HD)
    return h_out, k_out.reshape(shape), v_out.reshape(shape)


def solution(mesh):
    row_spec = P('dp', 'dm')
    cache_spec = P(('dp', 'dm'), None, 'tp', None)
    batch_spec = P(('dp', 'dm'))
    rope_spec = P(('dp', 'dm'), None)
    in_specs = (row_spec, P('dm', 'tp', None), P('dm', 'tp', None), P('dm', 'tp', None), P('tp', None, 'dm'), P('dm', 'tp'), P('dm', 'tp'), P('tp', 'dm'), P('dm'), P('dm'), cache_spec, cache_spec, batch_spec, rope_spec, rope_spec)
    return jax.shard_map(local_layer, mesh=mesh, in_specs=in_specs, out_specs=(row_spec, cache_spec, cache_spec), check_vma=False)
```
